256 devices in a mesh: inst: 4 (over y_hi, core), cells: 64 (over y_lo, x, z).
Axes of the slice: x: 4, y: 4 (y_hi: 2, y_lo: 2; y = y_hi * 2 + y_lo), z: 8, core: 2. Of those that a mesh axis runs over, the one named last changes fastest.
Arguments:
- flow_state: float32 [8, 5, 512, 32, 128], P('inst', None, 'cells'), may hold values from -6 to 6
- forcing: float32 [8, 5, 512, 32, 128], P('inst', None, 'cells'), may hold values from -6 to 6
- diffusion: float32 [512, 32, 128], P('cells'), may hold values from 0.2 to 0.6
- block_inverse: float32 [5, 5, 512, 32, 128], P(None, None, 'cells', 'inst'), may hold values from -0.03 to 0.15, as said below
Outputs:
- new_state: float32 [8, 5, 512, 32, 128], P('inst', None, 'cells')
The draws below stay inside these ranges and needn't reach their ends.
Inputs may be any that keep to these rules, and one draw needn't show every extreme that they name: block_inverse[v, v] lies between 0.06 and 0.15; entries off the diagonal lie between -0.03 and 0.03.
All inputs are finite; a program needn't handle non-finite values.
Results may differ from the reference program's by a relative error of at most 0.0001.
Values sent between devices are 32-bit elements; how exact they have to be, the bound alone decides.
No kernel may reach another device: no remote copies, remote signals or barrier semaphores. Data moves between devices by JAX's collectives and lax.ppermute only.
A program may use at most 64 MiB of HBM per device.

```python
import math
import jax
import jax.numpy as jnp
from jax import lax

INSTANCES = 8
VARIABLES = 5
NZ = 128
SWEEPS = 4
NX = 512
NY = 32


def draw_block_inverse(key, part):
    first_key, second_key = jax.random.split(jax.random.fold_in(key, 17))
    shape = (VARIABLES, VARIABLES, NX, NY, NZ)
    diagonal_vals = 0.06 * jnp.exp(jax.random.uniform(first_key, shape) * math.log(2.5))
    off_vals = jnp.clip(0.012 * jax.random.normal(second_key, shape), -0.03, 0.03)
    identity = jnp.eye(VARIABLES)[:, :, None, None, None]
    return jnp.where(identity > 0.5, diagonal_vals, off_vals).astype(jnp.float32)


def block_levels(key, shape, cuts, smallest, top_value):
    def one(dim, parts):
        steps = jax.random.uniform(jax.random.fold_in(jax.random.fold_in(key, 6), dim), (parts,), jnp.float32, smallest / len(cuts), top_value / len(cuts))
        return jnp.repeat(jnp.exp(steps), shape[dim] // parts).reshape((-1,) + (1,) * (len(shape) - dim - 1))

    loudness = one(*cuts[0])
    for cut in cuts[1:]:
        loudness = loudness * one(*cut)
    return loudness


def noise(own_key, dims, spread, most, cuts=(), held_as=jnp.bfloat16):
    values = jax.random.normal(own_key, dims, jnp.float32) * spread
    if len(cuts) > 0:
        values = block_levels(own_key, dims, cuts, -0.22, 0.18) * values
    return jnp.clip(values, min=-most, max=most).astype(held_as)


def setup_inputs(seed: int = 0) -> dict:
    arg_keys = jax.random.split(jax.random.key(seed), 5)
    return {
        "flow_state": noise(arg_keys[0], (INSTANCES, VARIABLES, NX, NY, NZ), 1.0, 6.0, ((0, 4), (2, 64)), jnp.float32),
        "forcing": noise(arg_keys[1], (INSTANCES, VARIABLES, NX, NY, NZ), 1.0, 6.0, ((0, 4), (2, 64)), jnp.float32),
        "diffusion": jnp.clip(jnp.exp(math.log(0.6) - 1.0986123 * jax.random.uniform(arg_keys[2], (NX, NY, NZ), jnp.float32) ** block_levels(arg_keys[2], (NX, NY, NZ), ((0, 64),), -0.2, 0.2)), 0.2, 0.6),
        "block_inverse": draw_block_inverse(jax.random.fold_in(arg_keys[4], 71), 0),
    }


frequency = 1.0


def spectral_matrix(count):
    index = jnp.arange(count)
    offset = index[:, None] - index[None, :]
    parity = jnp.where(offset % 2 == 0, 1.0, -1.0)
    angle = math.pi * jnp.where(offset == 0, 1, offset) / count
    entries = 0.5 * parity / jnp.tan(angle)
    return jnp.where(offset == 0, 0.0, entries).astype(jnp.float32)


def neighbour_sum(grid_field):
    padded = jnp.pad(grid_field, ((0, 0), (0, 0), (1, 1), (1, 1), (1, 1)))
    beside = padded[:, :, 2:, 1:-1, 1:-1] + padded[:, :, :-2, 1:-1, 1:-1]
    beside = beside + padded[:, :, 1:-1, 2:, 1:-1] + padded[:, :, 1:-1, :-2, 1:-1]
    beside = beside + padded[:, :, 1:-1, 1:-1, 2:] + padded[:, :, 1:-1, 1:-1, :-2]
    return beside


def spectral_term(matrix, grid_field):
    flat = grid_field.reshape(grid_field.shape[0], -1)
    product = jnp.dot(matrix, flat, precision=lax.Precision.HIGHEST)
    return (frequency * product).reshape(grid_field.shape)


def apply_blocks(block_inverse, source):
    return jnp.einsum("vwxyz,nwxyz->nvxyz", block_inverse, source, precision=lax.Precision.HIGHEST)


def reference(flow_state, forcing, diffusion, block_inverse):
    matrix = spectral_matrix(INSTANCES)
    weight = diffusion[None, None]
    residual = weight * (6.0 * flow_state - neighbour_sum(flow_state)) - forcing + spectral_term(matrix, flow_state)
    update = apply_blocks(block_inverse, -residual)
    for sweep_index in range(SWEEPS):
        source = -residual - spectral_term(matrix, update) + weight * neighbour_sum(update)
        update = apply_blocks(block_inverse, source)
    return flow_state + update
```

```python
import math

import jax
import jax.numpy as jnp
from jax import lax
from jax.experimental import pallas as pl
from jax.experimental.pallas import tpu as pltpu
from jax.sharding import PartitionSpec as P

AXES = ("inst", "cells")
NV = 5
RW = 20
BW = 24
F32 = jnp.float32


def place():
    index = lax.axis_index("inst")
    return index % 2, index // 2


def m8(value):
    return pl.multiple_of(value, 8)


def plane_of(s, core):
    return s + core * (7 - 2 * s)


def low_half():
    return lax.broadcasted_iota(jnp.int32, (8, 128), 0) < 4


def pack_rows(src, dst, offset, k, planes, core, chip):
    to_core = core ^ (k & 1)
    to_chip = chip ^ (k >> 1)
    low = low_half()

    def step(ev, carry):
        halo = []
        for si, s in enumerate(planes):
            base = (ev * 8 + plane_of(s, to_core)) * 32
            for t in range(2):
                dst[pl.ds(m8(offset + (ev * 2 + si) * 16 + 8 * t), 8), :] = src[
                    pl.ds(m8(base + 16 * to_chip + 8 * t), 8), :
                ]
            halo.append(src[pl.ds(m8(base + 16 - 8 * to_chip), 8), :])
        first, second = halo
        upper = jnp.where(low, first, pltpu.roll(second, 4, 0))
        lower = jnp.where(low, pltpu.roll(first, 4, 0), second)
        dst[pl.ds(m8(offset + 320 + ev * 8), 8), :] = jnp.where(to_chip == 1, lower, upper)
        return carry

    lax.fori_loop(0, 10, step, 0)


def state_kernel(f, o0, o1, o2, o3, first, last):
    core, chip = place()
    for k, out in ((2, o2), (3, o3), (1, o1), (0, o0)):
        pack_rows(f, out, 0, k, (0, 1), core, chip)
        pack_rows(f, out, 400, k, (2, 3), core, chip)

    def step(ev, carry):
        for t in range(4):
            first[pl.ds(m8(ev * 32 + 8 * t), 8), :] = f[pl.ds(m8(ev * 256 + 8 * t), 8), :]
            last[pl.ds(m8(ev * 32 + 8 * t), 8), :] = f[pl.ds(m8(ev * 256 + 224 + 8 * t), 8), :]
        return carry

    lax.fori_loop(0, 10, step, 0)


def part_kernel(f, g, d, lo, hi, e0, e1, e2, e3, i0, i1, i2, i3, part):
    core, chip = place()
    row = lax.broadcasted_iota(jnp.int32, (32, 128), 0)
    lane = lax.broadcasted_iota(jnp.int32, (32, 128), 1)

    def step(ev, carry):
        for x in range(8):
            own = f[pl.ds(m8((ev * 8 + x) * 32), 32), :]
            before = lo[pl.ds(m8(ev * 32), 32), :] if x == 0 else f[pl.ds(m8((ev * 8 + x - 1) * 32), 32), :]
            after = hi[pl.ds(m8(ev * 32), 32), :] if x == 7 else f[pl.ds(m8((ev * 8 + x + 1) * 32), 32), :]
            beside = before + after
            beside = beside + jnp.where(row == 0, 0.0, pltpu.roll(own, 1, 0))
            beside = beside + jnp.where(row == 31, 0.0, pltpu.roll(own, 31, 0))
            beside = beside + jnp.where(lane == 0, 0.0, pltpu.roll(own, 1, 1))
            beside = beside + jnp.where(lane == 127, 0.0, pltpu.roll(own, 127, 1))
            part[pl.ds(m8((ev * 8 + x) * 32), 32), :] = (
                d[pl.ds(x * 32, 32), :] * (6.0 * own - beside) - g[pl.ds(m8((ev * 8 + x) * 32), 32), :]
            )
        return carry

    lax.fori_loop(0, 10, step, 0)
    for k, out in ((2, e2), (3, e3), (1, e1), (0, e0)):
        pack_rows(part, out, 0, k, (0, 1), core, chip)
    for k, out in ((2, i2), (3, i3), (1, i1), (0, i0)):
        pack_rows(part, out, 0, k, (2, 3), core, chip)


ROOT8 = 1.0 / math.sqrt(8.0)
ROOT2 = 1.0 / math.sqrt(2.0)


def to_modes(pieces, core, chip):
    swapped = core == 1
    sums = [[pieces[a][e] + pieces[a + 2][e] for e in range(2)] for a in range(2)]
    diffs = [[pieces[a][e] - pieces[a + 2][e] for e in range(2)] for a in range(2)]
    s = [jnp.where(swapped, sums[1 - a][e], sums[a][e]) for a in range(2) for e in range(2)]
    d = [jnp.where(swapped, diffs[1 - a][e], diffs[a][e]) for a in range(2) for e in range(2)]
    half = jnp.where(chip == 1, -0.5, 0.5).astype(F32)
    even, odd = s[0] + s[2], s[1] + s[3]
    near, far = (d[1] - d[3]) * ROOT2, (d[1] + d[3]) * ROOT2
    return [
        half * (d[0] + near),
        0.5 * (s[0] - s[2]),
        half * (d[0] - near),
        ROOT8 * (even + odd),
        half * (far + d[2]),
        0.5 * (s[1] - s[3]),
        half * (far - d[2]),
        ROOT8 * (even - odd),
    ]


def from_modes(m):
    c1, c2, c3, m0, s1, s2, s3, m4 = m
    even, odd = ROOT8 * (m0 + m4), ROOT8 * (m0 - m4)
    s = [even + 0.5 * c2, odd + 0.5 * s2, even - 0.5 * c2, odd - 0.5 * s2]
    near, far = (0.5 * ROOT2) * (c1 - c3), (0.5 * ROOT2) * (s1 + s3)
    d = [0.5 * (c1 + c3), near + far, 0.5 * (s1 - s3), far - near]
    return [s[j] + d[j] for j in range(4)] + [s[j] - d[j] for j in range(4)]


def modes_kernel(offset, f0, f1, f2, f3, p0, p1, p2, p3, out):
    core, chip = place()
    fs, ps = (f0, f1, f2, f3), (p0, p1, p2, p3)

    def residual(row):
        mf = to_modes([[f[pl.ds(m8(offset + row + e * shift), 8), :] for e in range(2)] for f in fs], core, chip)
        mp = to_modes([[p[pl.ds(m8(row + e * shift), 8), :] for e in range(2)] for p in ps], core, chip)
        for k in range(3):
            mp[k] = mp[k] + (k + 1.0) * mf[4 + k]
            mp[4 + k] = mp[4 + k] - (k + 1.0) * mf[k]
        return mp

    def step(v, carry):
        nonlocal shift
        for si in range(2):
            for t in range(2):
                shift = 160
                modes = residual((v * 2 + si) * 16 + 8 * t)
                start = (si * RW + 4 * chip + 8 * t) * 40 + v * 8
                for m in range(8):
                    out[pl.ds(start + m, 8, stride=40), :] = modes[m]
        shift = 40
        modes = residual(320 + v * 8)
        for si in range(2):
            start = (si * RW + 16 * (1 - chip)) * 40 + v * 8
            for m in range(8):
                out[pl.ds(start + m, 4, stride=40), :] = modes[m][4 * si : 4 * si + 4, :]
        return carry

    shift = 160
    lax.fori_loop(0, NV, step, 0)


def inverse_pack_kernel(b, own, other, halo2, halo3):
    core, chip = place()
    low = low_half()

    def step(j, carry):
        for k, full, halo in ((0, own, halo2), (1, other, halo3)):
            rows = [b[pl.ds(m8((j * 8 + plane_of(s, core ^ k)) * 8), 8), :] for s in range(4)]
            for s in range(4):
                full[pl.ds(m8((j * 4 + s) * 8), 8), :] = rows[s]
            for a in range(2):
                first, second = rows[2 * a], rows[2 * a + 1]
                upper = jnp.where(low, first, pltpu.roll(second, 4, 0))
                lower = jnp.where(low, pltpu.roll(first, 4, 0), second)
                halo[pl.ds(m8((j * 2 + a) * 8), 8), :] = jnp.where(chip == 0, lower, upper)
        return carry

    lax.fori_loop(0, 25, step, 0)


def inverse_window_kernel(own, other, halo2, halo3, d, edge, inner):
    core, chip = place()
    low = low_half()
    straight = core == chip

    def step(j, carry):
        for s in range(4):
            out, base = (edge, inner)[s // 2], (j * 2 + s % 2) * BW
            out[pl.ds(m8(base + 8 * chip + 8 * core), 8), :] = own[pl.ds(m8((j * 4 + s) * 8), 8), :]
            out[pl.ds(m8(base + 8 * chip + 8 * (1 - core)), 8), :] = other[pl.ds(m8((j * 4 + s) * 8), 8), :]
        for a in range(2):
            at = pl.ds(m8((j * 2 + a) * 8), 8)
            both = jnp.where(straight, halo2[at, :], halo3[at, :])
            turned = pltpu.roll(both, 4, 0)
            out = (edge, inner)[a]
            for si in range(2):
                rows = jnp.where((chip == 0) == (si == 0), both, turned)
                rows = jnp.where(low == (chip == 0), rows, 0.0)
                out[pl.ds(m8((j * 2 + si) * BW + 16 * (1 - chip)), 8), :] = rows
        return carry

    lax.fori_loop(0, 25, step, 0)
    for s in range(4):
        out, base = (edge, inner)[s // 2], (25 * 2 + s % 2) * BW
        out[pl.ds(base, BW), :] = d[pl.ds(m8(plane_of(s, core) * 32 + 8 * chip), BW), :]


class Window:
    def __init__(self, beyond, edge, inner, across):
        self.at = [(beyond, 1), (beyond, 0), (edge, 0), (edge, 1), (inner, 0), (inner, 1), (across, 1), (across, 0)]


def wave_numbers():
    sub = lax.broadcasted_iota(jnp.int32, (8, 128), 0)
    rate = jnp.where(sub < 3, sub + 1, jnp.where(sub < 4, 0, jnp.where(sub < 7, 3 - sub, 0)))
    return rate.astype(F32)


def blocks(ref, s, row, source):
    def entry(j):
        return ref[pl.ds((j * 2 + s) * BW + row, 8, stride=0), :]

    outs = []
    for v in range(NV):
        total = entry(v * NV) * source[0]
        for u in range(1, NV):
            total = total + entry(v * NV + u) * source[u]
        outs.append(total)
    return outs


def sweep(planes, first, count, chip, resid, inv, u_in, write):
    lane = lax.broadcasted_iota(jnp.int32, (8, 128), 1)
    inside_low, inside_high = lane > 0, lane < 127
    rate = wave_numbers()

    def at(x, row, v):
        return u_in[(x * (RW + 2) + row + 1) * NV + v]

    def step(n, carry):
        row = first + n
        before = [at(planes[0] - 1, row, v) for v in range(NV)]
        own = [at(planes[0], row, v) for v in range(NV)]
        for x in planes:
            r_ref, s = resid.at[x]
            b_ref, _ = inv.at[x]
            weight = b_ref[pl.ds((25 * 2 + s) * BW + row + 4 * chip, 8, stride=0), :]
            after = [at(x + 1, row, v) for v in range(NV)]
            source = []
            for v in range(NV):
                w = own[v]
                beside = (before[v] + after[v]) + (at(x, row - 1, v) + at(x, row + 1, v))
                beside = beside + jnp.where(inside_low, pltpu.roll(w, 1, 1), 0.0)
                beside = beside + jnp.where(inside_high, pltpu.roll(w, 127, 1), 0.0)
                turned = r_ref[(s * RW + row) * NV + v] - rate * pltpu.roll(w, 4, 0)
                source.append(turned + weight * beside)
            write(x, row, blocks(b_ref, s, row + 4 * chip, source))
            before, own = own, after
        return carry

    lax.fori_loop(0, count, step, 0)


def clear_rows(u):
    zero = jnp.zeros((8, 128), F32)
    for x in range(8):
        for v in range(NV):
            u[x * (RW + 2) * NV + v] = zero
            u[(x * (RW + 2) + RW + 1) * NV + v] = zero


def into(u):
    def write(x, row, values):
        for v in range(NV):
            u[(x * (RW + 2) + row + 1) * NV + v] = values[v]

    return write


def first_kernel(rx, re, ri, rd, bx, be, bi, bd, edge, inner, u0, u1):
    _, chip = place()
    resid, inv = Window(rx, re, ri, rd), Window(bx, be, bi, bd)
    clear_rows(u0)
    clear_rows(u1)

    def step(row, carry):
        for x in range(8):
            r_ref, s = resid.at[x]
            b_ref, _ = inv.at[x]
            source = [r_ref[(s * RW + row) * NV + v] for v in range(NV)]
            into(u0)(x, row, blocks(b_ref, s, row + 4 * chip, source))
        return carry

    lax.fori_loop(0, RW, step, 0)
    sweep(range(1, 7), chip, RW - 1, chip, resid, inv, u0, into(u1))

    def write(x, row, values):
        out, s = (edge, x - 2) if x < 4 else (inner, x - 4)
        for v in range(NV):
            out[(s * (RW - 2) + row - 2 * chip) * NV + v] = values[v]

    sweep(range(2, 6), 2 * chip, RW - 2, chip, resid, inv, u1, write)


def second_kernel(rx, re, ri, rd, bx, be, bi, bd, ux, ue, ui, ud, o0, o1, o2, o3, u0, u1, last):
    core, chip = place()
    resid, inv = Window(rx, re, ri, rd), Window(bx, be, bi, bd)
    given = Window(ux, ue, ui, ud)
    clear_rows(u0)
    clear_rows(u1)

    def fill(n, carry):
        for x in range(8):
            ref, s = given.at[x]
            for v in range(NV):
                u0[(x * (RW + 2) + n + 2 * chip + 1) * NV + v] = ref[(s * (RW - 2) + n) * NV + v]
        return carry

    lax.fori_loop(0, RW - 2, fill, 0)
    sweep(range(1, 7), 3 * chip, RW - 3, chip, resid, inv, u0, into(u1))

    def write(x, row, values):
        for v in range(NV):
            last[pl.ds(m8((((x - 2) * 16 + row - 4 * chip) * NV + v) * 8), 8), :] = values[v]

    sweep(range(2, 6), 4 * chip, RW - 4, chip, resid, inv, u1, write)

    def unpack(v, carry):
        for s in range(4):
            for t in range(2):
                start = (s * 16 + 8 * t) * 40 + v * 8
                values = from_modes([last[pl.ds(start + m, 8, stride=40), :] for m in range(8)])
                pairs = [values[2 * q : 2 * q + 2] for q in range(4)]
                turned = [[jnp.where(core == 1, pairs[q ^ 1][e], pairs[q][e]) for e in range(2)] for q in range(4)]
                for k, out in enumerate((o0, o1, o2, o3)):
                    for e in range(2):
                        out[pl.ds(m8(((e * NV + v) * 4 + s) * 16 + 8 * t), 8), :] = jnp.where(
                            chip == 1, turned[k ^ 2][e], turned[k][e]
                        )
        return carry

    lax.fori_loop(0, NV, unpack, 0)


def final_kernel(f, w0, w1, w2, w3, out):
    core, chip = place()

    def step(ev, carry):
        for k, w in enumerate((w0, w1, w2, w3)):
            for s in range(4):
                base = (ev * 8 + plane_of(s, core ^ (k & 1))) * 32 + 16 * (chip ^ (k >> 1))
                for t in range(2):
                    at = pl.ds(m8(base + 8 * t), 8)
                    out[at, :] = f[at, :] - w[pl.ds(m8((ev * 4 + s) * 16 + 8 * t), 8), :]
        return carry

    lax.fori_loop(0, 10, step, 0)


def call(kernel, name, shapes, *args, scratch=()):
    return pl.pallas_call(
        kernel,
        name=name,
        out_shape=tuple(jax.ShapeDtypeStruct(s, F32) for s in shapes),
        scratch_shapes=[pltpu.VMEM(s, F32) for s in scratch],
        compiler_params=pltpu.CompilerParams(vmem_limit_bytes=40 * 1024 * 1024),
    )(*args)


def exchanges(cells):
    def pairs(move):
        found = []
        for i in range(4):
            for c in range(cells):
                target = move(i, c)
                if target is not None and 0 <= target[1] < cells:
                    found.append((i * cells + c, target[0] * cells + target[1]))
        return found

    return {
        "core": pairs(lambda i, c: (i ^ 1, c)),
        "chip": pairs(lambda i, c: (i ^ 2, c)),
        "both": pairs(lambda i, c: (i ^ 3, c)),
        "up": pairs(lambda i, c: (i, c + 1)),
        "down": pairs(lambda i, c: (i, c - 1)),
        "next": pairs(lambda i, c: (i ^ 1, c - 1 if i % 2 == 0 else c + 1)),
        "halo2": pairs(lambda i, c: (i ^ 2, c) if i in (1, 2) else None),
        "halo3": pairs(lambda i, c: (i ^ 3, c) if i in (1, 2) else None),
    }


def on_device(flow_state, forcing, diffusion, block_inverse):
    routes = exchanges(lax.axis_size("cells"))

    def send(value, route):
        return lax.ppermute(value, AXES, routes[route])

    f = flow_state.reshape(2560, 128)
    g = forcing.reshape(2560, 128)
    d = diffusion.reshape(256, 128)
    b = block_inverse.reshape(1600, 128)

    f0, f1, f2, f3, low, high = call(state_kernel, "state", [(800, 128)] * 4 + [(320, 128)] * 2, f)
    lo, hi = send(high, "up"), send(low, "down")
    f2, f3, f1 = send(f2, "chip"), send(f3, "both"), send(f1, "core")

    own, other, halo2, halo3 = call(
        inverse_pack_kernel, "inverse_pack", [(800, 128)] * 2 + [(400, 128)] * 2, b
    )
    other, halo2, halo3 = send(other, "core"), send(halo2, "halo2"), send(halo3, "halo3")

    parts = call(part_kernel, "part", [(400, 128)] * 8, f, g, d, lo, hi, scratch=[(2560, 128)])
    e0, e1, e2, e3, i0, i1, i2, i3 = parts
    e2, e3, e1 = send(e2, "chip"), send(e3, "both"), send(e1, "core")
    i2, i3, i1 = send(i2, "chip"), send(i3, "both"), send(i1, "core")

    be, bi = call(inverse_window_kernel, "inverse_window", [(26 * 2 * BW, 128)] * 2, own, other, halo2, halo3, d)
    bx, bd = send(be, "next"), send(bi, "core")

    (re,) = call(lambda *refs: modes_kernel(0, *refs), "modes_edge", [(2 * RW * 40, 128)], f0, f1, f2, f3, e0, e1, e2, e3)
    rx = send(re, "next")
    (ri,) = call(lambda *refs: modes_kernel(400, *refs), "modes_inner", [(2 * RW * 40, 128)], f0, f1, f2, f3, i0, i1, i2, i3)
    rd = send(ri, "core")

    resid = [r.reshape(2 * RW * NV, 8, 128) for r in (rx, re, ri, rd)]
    inv = (bx, be, bi, bd)
    u_shape = (8 * (RW + 2) * NV, 8, 128)
    ue, ui = call(
        first_kernel, "first", [(2 * (RW - 2) * NV, 8, 128)] * 2, *resid, *inv, scratch=[u_shape] * 2
    )
    ux, ud = send(ue, "next"), send(ui, "core")
    w0, w1, w2, w3 = call(
        second_kernel,
        "second",
        [(640, 128)] * 4,
        *resid,
        *inv,
        ux,
        ue,
        ui,
        ud,
        scratch=[u_shape] * 2 + [(4 * 16 * 40, 128)],
    )
    w2, w3, w1 = send(w2, "chip"), send(w3, "both"), send(w1, "core")
    (out,) = call(final_kernel, "final", [(2560, 128)], f, w0, w1, w2, w3)
    return out.reshape(flow_state.shape)


def solution(mesh):
    in_specs = (
        P("inst", None, "cells", None, None),
        P("inst", None, "cells", None, None),
        P("cells", None, None),
        P(None, None, "cells", "inst", None),
    )
    out_specs = P("inst", None, "cells", None, None)
    return jax.shard_map(
        on_device, mesh=mesh, in_specs=in_specs, out_specs=out_specs, check_vma=False
    )
```

```python
import math

import jax
import jax.numpy as jnp
from jax import lax
from jax.experimental import pallas as pl
from jax.experimental.pallas import tpu as pltpu
from jax.sharding import PartitionSpec as P


AXES = ("inst", "cells")
NV = 5
RW = 20
BW = 24
F32 = jnp.float32


def place():
    index = lax.axis_index("inst")
    return index % 2, index // 2


def m8(value):
    return pl.multiple_of(value, 8)


def plane_of(s, core):
    return s + core * (7 - 2 * s)


def low_half():
    return lax.broadcasted_iota(jnp.int32, (8, 128), 0) < 4


def pack_rows(src, dst, offset, k, planes, core, chip):
    to_core = core ^ (k & 1)
    to_chip = chip ^ (k >> 1)
    low = low_half()

    def step(ev, carry):
        halo = []
        for si, s in enumerate(planes):
            base = (ev * 8 + plane_of(s, to_core)) * 32
            for t in range(2):
                dst[pl.ds(m8(offset + (ev * 2 + si) * 16 + 8 * t), 8), :] = src[
                    pl.ds(m8(base + 16 * to_chip + 8 * t), 8), :
                ]
            halo.append(src[pl.ds(m8(base + 16 - 8 * to_chip), 8), :])
        first, second = halo
        upper = jnp.where(low, first, pltpu.roll(second, 4, 0))
        lower = jnp.where(low, pltpu.roll(first, 4, 0), second)
        dst[pl.ds(m8(offset + 320 + ev * 8), 8), :] = jnp.where(to_chip == 1, lower, upper)
        return carry

    lax.fori_loop(0, 10, step, 0)


def halo_kernel(own, other, out):
    core, chip = place()
    low = low_half()

    def step(j, carry):
        for a in range(2):
            at = [pl.ds(m8((j * 4 + 2 * a + si) * 8), 8) for si in range(2)]
            rows = [jnp.where(core == chip, other[x, :], own[x, :]) for x in at]
            upper = jnp.where(low, rows[0], pltpu.roll(rows[1], 4, 0))
            lower = jnp.where(low, pltpu.roll(rows[0], 4, 0), rows[1])
            out[pl.ds(m8((j * 2 + a) * 8), 8), :] = jnp.where(chip == 0, lower, upper)
        return carry

    lax.fori_loop(0, 25, step, 0)


def state_kernel(f, o0, o1, o2, o3, first, last):
    core, chip = place()
    for k, out in ((2, o2), (3, o3), (1, o1), (0, o0)):
        pack_rows(f, out, 0, k, (0, 1), core, chip)
        pack_rows(f, out, 400, k, (2, 3), core, chip)

    def step(ev, carry):
        for t in range(4):
            first[pl.ds(m8(ev * 32 + 8 * t), 8), :] = f[pl.ds(m8(ev * 256 + 8 * t), 8), :]
            last[pl.ds(m8(ev * 32 + 8 * t), 8), :] = f[pl.ds(m8(ev * 256 + 224 + 8 * t), 8), :]
        return carry

    lax.fori_loop(0, 10, step, 0)


def part_kernel(f, g, d, lo, hi, e0, e1, e2, e3, i0, i1, i2, i3, part):
    core, chip = place()
    row = lax.broadcasted_iota(jnp.int32, (32, 128), 0)
    lane = lax.broadcasted_iota(jnp.int32, (32, 128), 1)

    def step(ev, carry):
        for x in range(8):
            own = f[pl.ds(m8((ev * 8 + x) * 32), 32), :]
            before = lo[pl.ds(m8(ev * 32), 32), :] if x == 0 else f[pl.ds(m8((ev * 8 + x - 1) * 32), 32), :]
            after = hi[pl.ds(m8(ev * 32), 32), :] if x == 7 else f[pl.ds(m8((ev * 8 + x + 1) * 32), 32), :]
            beside = before + after
            beside = beside + jnp.where(row == 0, 0.0, pltpu.roll(own, 1, 0))
            beside = beside + jnp.where(row == 31, 0.0, pltpu.roll(own, 31, 0))
            beside = beside + jnp.where(lane == 0, 0.0, pltpu.roll(own, 1, 1))
            beside = beside + jnp.where(lane == 127, 0.0, pltpu.roll(own, 127, 1))
            part[pl.ds(m8((ev * 8 + x) * 32), 32), :] = (
                d[pl.ds(x * 32, 32), :] * (6.0 * own - beside) - g[pl.ds(m8((ev * 8 + x) * 32), 32), :]
            )
        return carry

    lax.fori_loop(0, 10, step, 0)
    for k, out in ((2, e2), (3, e3), (1, e1), (0, e0)):
        pack_rows(part, out, 0, k, (0, 1), core, chip)
    for k, out in ((2, i2), (3, i3), (1, i1), (0, i0)):
        pack_rows(part, out, 0, k, (2, 3), core, chip)


ROOT8 = 1.0 / math.sqrt(8.0)
ROOT2 = 1.0 / math.sqrt(2.0)


def to_modes(pieces, core, chip):
    swapped = core == 1
    sums = [[pieces[a][e] + pieces[a + 2][e] for e in range(2)] for a in range(2)]
    diffs = [[pieces[a][e] - pieces[a + 2][e] for e in range(2)] for a in range(2)]
    s = [jnp.where(swapped, sums[1 - a][e], sums[a][e]) for a in range(2) for e in range(2)]
    d = [jnp.where(swapped, diffs[1 - a][e], diffs[a][e]) for a in range(2) for e in range(2)]
    half = jnp.where(chip == 1, -0.5, 0.5).astype(F32)
    even, odd = s[0] + s[2], s[1] + s[3]
    near, far = (d[1] - d[3]) * ROOT2, (d[1] + d[3]) * ROOT2
    return [
        half * (d[0] + near),
        0.5 * (s[0] - s[2]),
        half * (d[0] - near),
        ROOT8 * (even + odd),
        half * (far + d[2]),
        0.5 * (s[1] - s[3]),
        half * (far - d[2]),
        ROOT8 * (even - odd),
    ]


def from_modes(m):
    c1, c2, c3, m0, s1, s2, s3, m4 = m
    even, odd = ROOT8 * (m0 + m4), ROOT8 * (m0 - m4)
    s = [even + 0.5 * c2, odd + 0.5 * s2, even - 0.5 * c2, odd - 0.5 * s2]
    near, far = (0.5 * ROOT2) * (c1 - c3), (0.5 * ROOT2) * (s1 + s3)
    d = [0.5 * (c1 + c3), near + far, 0.5 * (s1 - s3), far - near]
    return [s[j] + d[j] for j in range(4)] + [s[j] - d[j] for j in range(4)]


def edge_kernel(f0, f1, f2, f3, p0, p1, p2, p3, be, out, sent):
    _, chip = place()
    modes_kernel(0, f0, f1, f2, f3, p0, p1, p2, p3, out)

    def step(row, carry):
        at = [pl.ds(m8((row * NV + v) * 8), 8) for v in range(NV)]
        beside = [pl.ds(m8(((RW + row) * NV + v) * 8), 8) for v in range(NV)]
        values = blocks((be, 1, 2), row + 4 * chip, [out[b, :] for b in beside])
        for v in range(NV):
            sent[at[v], :] = out[at[v], :]
            sent[beside[v], :] = values[v]
        return carry

    lax.fori_loop(0, RW, step, 0, unroll=4)


def modes_kernel(offset, f0, f1, f2, f3, p0, p1, p2, p3, out):
    core, chip = place()
    fs, ps = (f0, f1, f2, f3), (p0, p1, p2, p3)

    def residual(row):
        mf = to_modes([[f[pl.ds(m8(offset + row + e * shift), 8), :] for e in range(2)] for f in fs], core, chip)
        mp = to_modes([[p[pl.ds(m8(row + e * shift), 8), :] for e in range(2)] for p in ps], core, chip)
        for k in range(3):
            mp[k] = mp[k] + (k + 1.0) * mf[4 + k]
            mp[4 + k] = mp[4 + k] - (k + 1.0) * mf[k]
        return mp

    def step(v, carry):
        nonlocal shift
        for si in range(2):
            for t in range(2):
                shift = 160
                modes = residual((v * 2 + si) * 16 + 8 * t)
                start = (si * RW + 4 * chip + 8 * t) * 40 + v * 8
                for m in range(8):
                    out[pl.ds(start + m, 8, stride=40), :] = modes[m]
        shift = 40
        modes = residual(320 + v * 8)
        for si in range(2):
            start = (si * RW + 16 * (1 - chip)) * 40 + v * 8
            for m in range(8):
                out[pl.ds(start + m, 4, stride=40), :] = modes[m][4 * si : 4 * si + 4, :]
        return carry

    shift = 160
    lax.fori_loop(0, NV, step, 0)


def inverse_pack_kernel(b, own, other):
    core, _ = place()

    def step(j, carry):
        for k, full in ((0, own), (1, other)):
            for s in range(4):
                full[pl.ds(m8((j * 4 + s) * 8), 8), :] = b[pl.ds(m8((j * 8 + plane_of(s, core ^ k)) * 8), 8), :]
        return carry

    lax.fori_loop(0, 25, step, 0)


def inverse_window_kernel(own, other, halo, d, edge, inner, outer):
    core, chip = place()
    low = low_half()

    def step(j, carry):
        for s in range(4):
            out, base = (edge, inner)[s // 2], (j * 2 + s % 2) * BW
            out[pl.ds(m8(base + 8 * chip + 8 * core), 8), :] = own[pl.ds(m8((j * 4 + s) * 8), 8), :]
            out[pl.ds(m8(base + 8 * chip + 8 * (1 - core)), 8), :] = other[pl.ds(m8((j * 4 + s) * 8), 8), :]
        for a in range(2):
            both = halo[pl.ds(m8((j * 2 + a) * 8), 8), :]
            turned = pltpu.roll(both, 4, 0)
            out = (edge, inner)[a]
            for si in range(2):
                rows = jnp.where((chip == 0) == (si == 0), both, turned)
                rows = jnp.where(low == (chip == 0), rows, 0.0)
                out[pl.ds(m8((j * 2 + si) * BW + 16 * (1 - chip)), 8), :] = rows
        return carry

    lax.fori_loop(0, 25, step, 0)
    for s in range(4):
        out, base = (edge, inner)[s // 2], (25 * 2 + s % 2) * BW
        out[pl.ds(base, BW), :] = d[pl.ds(m8(plane_of(s, core) * 32 + 8 * chip), BW), :]

    def copy(j, carry):
        for t in range(BW // 8):
            outer[pl.ds(m8(j * BW + 8 * t), 8), :] = edge[pl.ds(m8(j * 2 * BW + 8 * t), 8), :]
        return carry

    lax.fori_loop(0, 26, copy, 0)


def wave_numbers():
    sub = lax.broadcasted_iota(jnp.int32, (8, 128), 0)
    rate = jnp.where(sub < 3, sub + 1, jnp.where(sub < 4, 0, jnp.where(sub < 7, 3 - sub, 0)))
    return rate.astype(F32)


def blocks(place, row, source):
    ref, s, count = place

    def entry(j):
        return ref[pl.ds((j * count + s) * BW + row, 8, stride=0), :]

    outs = []
    for v in range(NV):
        total = entry(v * NV) * source[0]
        for u in range(1, NV):
            total = total + entry(v * NV + u) * source[u]
        outs.append(total)
    return outs


def eight(beyond, edge, inner, across):
    kept = ((beyond, 1), (beyond, 0), (edge, 0), (edge, 1), (inner, 0), (inner, 1), (across, 1), (across, 0))
    return {x: at for x, at in enumerate(kept) if at[0] is not None}


def inverses(beyond, edge, inner, across):
    held = {x: (ref, s, 2) for x, (ref, s) in eight(None, edge, inner, across).items()}
    return held | {1: (beyond, 0, 1)}


def residuals(beyond, edge, inner, across):
    held = eight(beyond, edge, inner, across)
    return {x: at for x, at in held.items() if x > 0}


def first_solve(planes, chip, resid, inv, write):
    def step(row, carry):
        for x in planes:
            ref, s = resid[x]
            source = [ref[(s * RW + row) * NV + v] for v in range(NV)]
            write(x, row, blocks(inv[x], row + 4 * chip, source))
        return carry

    lax.fori_loop(0, RW, step, 0, unroll=4)


def sweep(planes, first, count, chip, resid, inv, update, write):
    lane = lax.broadcasted_iota(jnp.int32, (8, 128), 1)
    inside_low, inside_high = lane > 0, lane < 127
    rate = wave_numbers()

    def at(x, row, v):
        ref, s = update[x]
        return ref[(s * (RW + 2) + row + 1) * NV + v]

    def step(n, carry):
        row = first + n
        before = [at(planes[0] - 1, row, v) for v in range(NV)]
        own = [at(planes[0], row, v) for v in range(NV)]
        for x in planes:
            r_ref, s = resid[x]
            b_ref, b_s, b_count = inv[x]
            weight = b_ref[pl.ds((25 * b_count + b_s) * BW + row + 4 * chip, 8, stride=0), :]
            after = [at(x + 1, row, v) for v in range(NV)]
            source = []
            for v in range(NV):
                w = own[v]
                beside = (before[v] + after[v]) + (at(x, row - 1, v) + at(x, row + 1, v))
                beside = beside + jnp.where(inside_low, pltpu.roll(w, 1, 1), 0.0)
                beside = beside + jnp.where(inside_high, pltpu.roll(w, 127, 1), 0.0)
                turned = r_ref[(s * RW + row) * NV + v] - rate * pltpu.roll(w, 4, 0)
                source.append(turned + weight * beside)
            write(x, row, blocks(inv[x], row + 4 * chip, source))
            before, own = own, after
        return carry

    lax.fori_loop(0, count, step, 0, unroll=6 if count % 6 == 0 else 4)


def clear_rows(*refs):
    zero = jnp.zeros((8, 128), F32)
    for ref in refs:
        for x in range(ref.shape[0] // ((RW + 2) * NV)):
            for v in range(NV):
                ref[x * (RW + 2) * NV + v] = zero
                ref[(x * (RW + 2) + RW + 1) * NV + v] = zero


def into(update):
    def write(x, row, values):
        ref, s = update[x]
        for v in range(NV):
            ref[(s * (RW + 2) + row + 1) * NV + v] = values[v]

    return write


def into_edge(out, start, chip):
    def write(x, row, values):
        for v in range(NV):
            out[((x - start) * (RW - 2) + row - 2 * chip) * NV + v] = values[v]

    return write


def fill(update, given, chip):
    def step(n, carry):
        for x, (ref, s) in given.items():
            into(update)(x, n + 2 * chip, [ref[(s * (RW - 2) + n) * NV + v] for v in range(NV)])
        return carry

    lax.fori_loop(0, RW - 2, step, 0, unroll=3)


def first_inner_kernel(re, ri, rd, be, bi, bd, ui, k0, k1, u0, u1):
    _, chip = place()
    resid, inv = residuals(None, re, ri, rd), inverses(None, be, bi, bd)
    zeroth = {2: (k0, 0), 3: (k0, 1)} | {x: (u0, x - 4) for x in range(4, 8)}
    oneth = {3: (k1, 0), 4: (k1, 1), 5: (u1, 0), 6: (u1, 1)}
    clear_rows(u0, u1, k0, k1)
    first_solve(range(2, 8), chip, resid, inv, into(zeroth))
    sweep(range(3, 7), 0, RW, chip, resid, inv, zeroth, into(oneth))
    sweep(range(4, 6), 2 * chip, RW - 2, chip, resid, inv, oneth, into_edge(ui, 4, chip))


def first_edge_kernel(cells, rx, re, bx, by, be, k0, k1, ue, bz, u0, u1):
    core, chip = place()
    resid, inv = residuals(rx, re, None, None), inverses(bz, be, None, None)
    zeroth = {0: (u0, 0), 1: (u0, 1), 2: (k0, 0), 3: (k0, 1)}
    oneth = {1: (u1, 0), 2: (u1, 1), 3: (k1, 0), 4: (k1, 1)}
    clear_rows(u0, u1)
    passed_on = lax.axis_index("cells") == jnp.where(core == 0, 0, cells - 1)

    def copy(row, carry):
        into(zeroth)(0, row, [rx[(RW + row) * NV + v] for v in range(NV)])
        return carry

    def copy_blocks(j, carry):
        at = pl.ds(m8(j * 8), 8)
        bz[at, :] = by[at, :] + jnp.where(passed_on, 0.0, bx[at, :])
        return carry

    lax.fori_loop(0, RW, copy, 0, unroll=4)
    lax.fori_loop(0, 26 * BW // 8, copy_blocks, 0, unroll=6)
    first_solve(range(1, 2), chip, resid, inv, into(zeroth))
    sweep(range(1, 3), 0, RW, chip, resid, inv, zeroth, into(oneth))
    sweep(range(2, 4), 2 * chip, RW - 2, chip, resid, inv, oneth, into_edge(ue, 2, chip))


def unpack(last, outs, core, chip):
    def step(v, carry):
        for s in range(2):
            for t in range(2):
                start = (s * 16 + 8 * t) * 40 + v * 8
                values = from_modes([last[pl.ds(start + m, 8, stride=40), :] for m in range(8)])
                pairs = [values[2 * q : 2 * q + 2] for q in range(4)]
                turned = [[jnp.where(core == 1, pairs[q ^ 1][e], pairs[q][e]) for e in range(2)] for q in range(4)]
                for k, out in enumerate(outs):
                    for e in range(2):
                        out[pl.ds(m8(((e * NV + v) * 2 + s) * 16 + 8 * t), 8), :] = jnp.where(
                            chip == 1, turned[k ^ 2][e], turned[k][e]
                        )
        return carry

    lax.fori_loop(0, NV, step, 0)


def into_last(last, start, chip):
    def write(x, row, values):
        for v in range(NV):
            last[pl.ds(m8((((x - start) * 16 + row - 4 * chip) * NV + v) * 8), 8), :] = values[v]

    return write


def second_inner_kernel(re, ri, rd, be, bi, bd, ue, ui, ud, o0, o1, o2, o3, k3, u2, u3, last):
    core, chip = place()
    resid, inv = residuals(None, re, ri, rd), inverses(None, be, bi, bd)
    second = {x: (u2, x - 2) for x in range(2, 8)}
    third = {3: (k3, 0), 4: (k3, 1), 5: (u3, 0), 6: (u3, 1)}
    clear_rows(u2, u3, k3)
    fill(second, eight(None, ue, ui, ud), chip)
    sweep(range(3, 7), 2 * chip, RW - 2, chip, resid, inv, second, into(third))
    sweep(range(4, 6), 4 * chip, RW - 4, chip, resid, inv, third, into_last(last, 4, chip))
    unpack(last, (o0, o1, o2, o3), core, chip)


def second_edge_kernel(rx, re, bx, be, ux, ue, k3, o0, o1, o2, o3, u2, u3, last):
    core, chip = place()
    resid, inv = residuals(rx, re, None, None), inverses(bx, be, None, None)
    second = {x: (u2, x) for x in range(4)}
    third = {1: (u3, 0), 2: (u3, 1), 3: (k3, 0), 4: (k3, 1)}
    clear_rows(u2, u3)
    fill(second, eight(ux, ue, None, None), chip)
    sweep(range(1, 3), 2 * chip, RW - 2, chip, resid, inv, second, into(third))
    sweep(range(2, 4), 4 * chip, RW - 4, chip, resid, inv, third, into_last(last, 2, chip))
    unpack(last, (o0, o1, o2, o3), core, chip)


def final_kernel(f, w0, w1, w2, w3, v0, v1, v2, v3, out):
    core, chip = place()

    def step(ev, carry):
        for k in range(4):
            for s in range(4):
                w = ((w0, w1, w2, w3), (v0, v1, v2, v3))[s // 2][k]
                base = (ev * 8 + plane_of(s, core ^ (k & 1))) * 32 + 16 * (chip ^ (k >> 1))
                for t in range(2):
                    at = pl.ds(m8(base + 8 * t), 8)
                    out[at, :] = f[at, :] - w[pl.ds(m8((ev * 2 + s % 2) * 16 + 8 * t), 8), :]
        return carry

    lax.fori_loop(0, 10, step, 0)


def call(kernel, shapes, *args, scratch=()):
    return pl.pallas_call(
        kernel,
        out_shape=tuple(jax.ShapeDtypeStruct(s, F32) for s in shapes),
        scratch_shapes=[pltpu.VMEM(s, F32) for s in scratch],
        compiler_params=pltpu.CompilerParams(vmem_limit_bytes=40 * 1024 * 1024),
    )(*args)


def exchanges(cells):
    def pairs(move):
        found = []
        for i in range(4):
            for c in range(cells):
                target = move(i, c)
                if target is not None and 0 <= target[1] < cells:
                    found.append((i * cells + c, target[0] * cells + target[1]))
        return found

    def beside(i, c):
        return i ^ 1, c - 1 if i % 2 == 0 else c + 1

    half = cells // 2
    middle, ends = ((0, half), (1, half - 1)), (0, cells - 1)
    return {
        "core": pairs(lambda i, c: (i ^ 1, c)),
        "chip": pairs(lambda i, c: (i ^ 2, c)),
        "both": pairs(lambda i, c: (i ^ 3, c)),
        "up": pairs(lambda i, c: (i, c + 1)),
        "down": pairs(lambda i, c: (i, c - 1)),
        "next": pairs(beside),
        "leg": pairs(lambda i, c: (i ^ 1, ends[i % 2 ^ 1]) if (i % 2, c) in middle else beside(i, c)),
        "relay": pairs(lambda i, c: (i, half - i % 2) if c == ends[i % 2] else None),
    }


def on_device(flow_state, forcing, diffusion, block_inverse):
    routes = exchanges(lax.axis_size("cells"))

    def send(value, route):
        return lax.ppermute(value, AXES, routes[route])

    f = flow_state.reshape(2560, 128)
    g = forcing.reshape(2560, 128)
    d = diffusion.reshape(256, 128)
    b = block_inverse.reshape(1600, 128)

    states = [(800, 128)] * 4 + [(320, 128)] * 2
    f0, f1, f2, f3, low, high = call(state_kernel, states, f)
    f2, f3 = send(f2, "chip"), send(f3, "both")
    lo, hi = send(high, "up"), send(low, "down")
    own, other = call(inverse_pack_kernel, [(800, 128)] * 2, b)
    other = send(other, "core")
    f1 = send(f1, "core")
    (halo,) = call(halo_kernel, [(400, 128)], own, other)
    halo = send(halo, "chip")

    parts = call(part_kernel, [(400, 128)] * 8, f, g, d, lo, hi, scratch=[(2560, 128)])
    e0, e1, e2, e3, i0, i1, i2, i3 = parts
    e2, e3, e1 = send(e2, "chip"), send(e3, "both"), send(e1, "core")
    i2, i3, i1 = send(i2, "chip"), send(i3, "both"), send(i1, "core")

    windows = [(26 * 2 * BW, 128)] * 2 + [(26 * BW, 128)]
    be, bi, bx = call(inverse_window_kernel, windows, own, other, halo, d)
    bx, bd = send(bx, "leg"), send(bi, "core")

    r_shape = (2 * RW * 40, 128)
    re, rx = call(edge_kernel, [r_shape] * 2, f0, f1, f2, f3, e0, e1, e2, e3, be)
    rx = send(rx, "next")
    by = send(bx, "relay")
    (ri,) = call(lambda *refs: modes_kernel(400, *refs), [r_shape], f0, f1, f2, f3, i0, i1, i2, i3)
    rd = send(ri, "core")
    rx, re, ri, rd = (r.reshape(-1, 8, 128) for r in (rx, re, ri, rd))

    def planes(count):
        return (count * (RW + 2) * NV, 8, 128)

    u_shape, last = (2 * (RW - 2) * NV, 8, 128), (2 * 16 * 40, 128)
    ui, k0, k1 = call(
        first_inner_kernel, [u_shape, planes(2), planes(2)], *(re, ri, rd, be, bi, bd), scratch=[planes(4), planes(2)]
    )
    ud = send(ui, "core")
    cells = lax.axis_size("cells")
    ue, bx = call(
        lambda *refs: first_edge_kernel(cells, *refs),
        [u_shape, (26 * BW, 128)],
        *(rx, re, bx, by, be, k0, k1),
        scratch=[planes(2), planes(2)],
    )
    ux = send(ue, "next")
    v0, v1, v2, v3, k3 = call(
        second_inner_kernel,
        [(320, 128)] * 4 + [planes(2)],
        *(re, ri, rd, be, bi, bd, ue, ui, ud),
        scratch=[planes(6), planes(2), last],
    )
    v2, v3, v1 = send(v2, "chip"), send(v3, "both"), send(v1, "core")
    w0, w1, w2, w3 = call(
        second_edge_kernel, [(320, 128)] * 4, *(rx, re, bx, be, ux, ue, k3), scratch=[planes(4), planes(2), last]
    )
    w2, w3, w1 = send(w2, "chip"), send(w3, "both"), send(w1, "core")
    (out,) = call(final_kernel, [(2560, 128)], f, w0, w1, w2, w3, v0, v1, v2, v3)
    return out.reshape(flow_state.shape)


def solution(mesh):
    in_specs = (
        P("inst", None, "cells", None, None),
        P("inst", None, "cells", None, None),
        P("cells", None, None),
        P(None, None, "cells", "inst", None),
    )
    out_specs = P("inst", None, "cells", None, None)
    return jax.shard_map(
        on_device, mesh=mesh, in_specs=in_specs, out_specs=out_specs, check_vma=False
    )
```

```python
import math

import jax
import jax.numpy as jnp
from jax import lax
from jax.experimental import pallas as pl
from jax.experimental.pallas import tpu as pltpu
from jax.sharding import PartitionSpec as P


AXES = ("inst", "cells")
NV = 5
RW = 20
BW = 24
F32 = jnp.float32


def place():
    index = lax.axis_index("inst")
    return index % 2, index // 2


def m8(value):
    return pl.multiple_of(value, 8)


def plane_of(s, core):
    return s + core * (7 - 2 * s)


def low_half():
    return lax.broadcasted_iota(jnp.int32, (8, 128), 0) < 4


def pack_rows(src, dst, offset, k, planes, core, chip):
    to_core = core ^ (k & 1)
    to_chip = chip ^ (k >> 1)
    low = low_half()

    def step(ev, carry):
        halo = []
        for si, s in enumerate(planes):
            base = (ev * 8 + plane_of(s, to_core)) * 32
            for t in range(2):
                dst[pl.ds(m8(offset + (ev * 2 + si) * 16 + 8 * t), 8), :] = src[
                    pl.ds(m8(base + 16 * to_chip + 8 * t), 8), :
                ]
            halo.append(src[pl.ds(m8(base + 16 - 8 * to_chip), 8), :])
        first, second = halo
        upper = jnp.where(low, first, pltpu.roll(second, 4, 0))
        lower = jnp.where(low, pltpu.roll(first, 4, 0), second)
        dst[pl.ds(m8(offset + 320 + ev * 8), 8), :] = jnp.where(to_chip == 1, lower, upper)
        return carry

    lax.fori_loop(0, 10, step, 0)


def halo_kernel(own, other, out):
    core, chip = place()
    low = low_half()

    def step(j, carry):
        for a in range(2):
            at = [pl.ds(m8((j * 4 + 2 * a + si) * 8), 8) for si in range(2)]
            rows = [jnp.where(core == chip, other[x, :], own[x, :]) for x in at]
            upper = jnp.where(low, rows[0], pltpu.roll(rows[1], 4, 0))
            lower = jnp.where(low, pltpu.roll(rows[0], 4, 0), rows[1])
            out[pl.ds(m8((j * 2 + a) * 8), 8), :] = jnp.where(chip == 0, lower, upper)
        return carry

    lax.fori_loop(0, 25, step, 0)


def state_kernel(f, o0, o1, o2, o3, first, last):
    core, chip = place()
    for k, out in ((2, o2), (3, o3), (1, o1), (0, o0)):
        pack_rows(f, out, 0, k, (0, 1), core, chip)
        pack_rows(f, out, 400, k, (2, 3), core, chip)

    def step(ev, carry):
        for t in range(4):
            first[pl.ds(m8(ev * 32 + 8 * t), 8), :] = f[pl.ds(m8(ev * 256 + 8 * t), 8), :]
            last[pl.ds(m8(ev * 32 + 8 * t), 8), :] = f[pl.ds(m8(ev * 256 + 224 + 8 * t), 8), :]
        return carry

    lax.fori_loop(0, 10, step, 0)


def part_kernel(f, g, d, lo, hi, e0, e1, e2, e3, i0, i1, i2, i3, part):
    core, chip = place()
    row = lax.broadcasted_iota(jnp.int32, (32, 128), 0)
    lane = lax.broadcasted_iota(jnp.int32, (32, 128), 1)

    def step(ev, carry):
        for x in range(8):
            own = f[pl.ds(m8((ev * 8 + x) * 32), 32), :]
            before = lo[pl.ds(m8(ev * 32), 32), :] if x == 0 else f[pl.ds(m8((ev * 8 + x - 1) * 32), 32), :]
            after = hi[pl.ds(m8(ev * 32), 32), :] if x == 7 else f[pl.ds(m8((ev * 8 + x + 1) * 32), 32), :]
            beside = before + after
            beside = beside + jnp.where(row == 0, 0.0, pltpu.roll(own, 1, 0))
            beside = beside + jnp.where(row == 31, 0.0, pltpu.roll(own, 31, 0))
            beside = beside + jnp.where(lane == 0, 0.0, pltpu.roll(own, 1, 1))
            beside = beside + jnp.where(lane == 127, 0.0, pltpu.roll(own, 127, 1))
            part[pl.ds(m8((ev * 8 + x) * 32), 32), :] = (
                d[pl.ds(x * 32, 32), :] * (6.0 * own - beside) - g[pl.ds(m8((ev * 8 + x) * 32), 32), :]
            )
        return carry

    lax.fori_loop(0, 10, step, 0)
    for k, out in ((2, e2), (3, e3), (1, e1), (0, e0)):
        pack_rows(part, out, 0, k, (0, 1), core, chip)
    for k, out in ((2, i2), (3, i3), (1, i1), (0, i0)):
        pack_rows(part, out, 0, k, (2, 3), core, chip)


ROOT8 = 1.0 / math.sqrt(8.0)
ROOT2 = 1.0 / math.sqrt(2.0)


def to_modes(pieces, core, chip):
    swapped = core == 1
    sums = [[pieces[a][e] + pieces[a + 2][e] for e in range(2)] for a in range(2)]
    diffs = [[pieces[a][e] - pieces[a + 2][e] for e in range(2)] for a in range(2)]
    s = [jnp.where(swapped, sums[1 - a][e], sums[a][e]) for a in range(2) for e in range(2)]
    d = [jnp.where(swapped, diffs[1 - a][e], diffs[a][e]) for a in range(2) for e in range(2)]
    half = jnp.where(chip == 1, -0.5, 0.5).astype(F32)
    even, odd = s[0] + s[2], s[1] + s[3]
    near, far = (d[1] - d[3]) * ROOT2, (d[1] + d[3]) * ROOT2
    return [
        half * (d[0] + near),
        0.5 * (s[0] - s[2]),
        half * (d[0] - near),
        ROOT8 * (even + odd),
        half * (far + d[2]),
        0.5 * (s[1] - s[3]),
        half * (far - d[2]),
        ROOT8 * (even - odd),
    ]


def from_modes(m):
    c1, c2, c3, m0, s1, s2, s3, m4 = m
    even, odd = ROOT8 * (m0 + m4), ROOT8 * (m0 - m4)
    s = [even + 0.5 * c2, odd + 0.5 * s2, even - 0.5 * c2, odd - 0.5 * s2]
    near, far = (0.5 * ROOT2) * (c1 - c3), (0.5 * ROOT2) * (s1 + s3)
    d = [0.5 * (c1 + c3), near + far, 0.5 * (s1 - s3), far - near]
    return [s[j] + d[j] for j in range(4)] + [s[j] - d[j] for j in range(4)]


def edge_kernel(f0, f1, f2, f3, p0, p1, p2, p3, be, out, sent):
    _, chip = place()
    modes_kernel(0, f0, f1, f2, f3, p0, p1, p2, p3, out)

    def tile(row, v):
        return pl.ds(m8((row * NV + v) * 8), 8)

    for n in range(RW - 1):
        for v in range(NV):
            sent[tile(n, v), :] = out[tile(n + chip, v), :]

    def step(n, carry):
        row = n + 2 * chip
        values = blocks((be, 1, 2), row + 4 * chip, [out[tile(RW + row, v), :] for v in range(NV)])
        for v in range(NV):
            sent[tile(RW - 1 + n, v), :] = values[v]
        return carry

    lax.fori_loop(0, RW - 2, step, 0, unroll=6)


def modes_kernel(offset, f0, f1, f2, f3, p0, p1, p2, p3, out):
    core, chip = place()
    fs, ps = (f0, f1, f2, f3), (p0, p1, p2, p3)

    def residual(row):
        mf = to_modes([[f[pl.ds(m8(offset + row + e * shift), 8), :] for e in range(2)] for f in fs], core, chip)
        mp = to_modes([[p[pl.ds(m8(row + e * shift), 8), :] for e in range(2)] for p in ps], core, chip)
        for k in range(3):
            mp[k] = mp[k] + (k + 1.0) * mf[4 + k]
            mp[4 + k] = mp[4 + k] - (k + 1.0) * mf[k]
        return mp

    def step(v, carry):
        nonlocal shift
        for si in range(2):
            for t in range(2):
                shift = 160
                modes = residual((v * 2 + si) * 16 + 8 * t)
                start = (si * RW + 4 * chip + 8 * t) * 40 + v * 8
                for m in range(8):
                    out[pl.ds(start + m, 8, stride=40), :] = modes[m]
        shift = 40
        modes = residual(320 + v * 8)
        for si in range(2):
            start = (si * RW + 16 * (1 - chip)) * 40 + v * 8
            for m in range(8):
                out[pl.ds(start + m, 4, stride=40), :] = modes[m][4 * si : 4 * si + 4, :]
        return carry

    shift = 160
    lax.fori_loop(0, NV, step, 0)


def inverse_pack_kernel(b, own, other):
    core, _ = place()

    def step(j, carry):
        for k, full in ((0, own), (1, other)):
            for s in range(4):
                full[pl.ds(m8((j * 4 + s) * 8), 8), :] = b[pl.ds(m8((j * 8 + plane_of(s, core ^ k)) * 8), 8), :]
        return carry

    lax.fori_loop(0, 25, step, 0)


def inverse_window_kernel(own, other, halo, d, edge, inner, outer):
    core, chip = place()
    low = low_half()

    def step(j, carry):
        for s in range(4):
            out, base = (edge, inner)[s // 2], (j * 2 + s % 2) * BW
            out[pl.ds(m8(base + 8 * chip + 8 * core), 8), :] = own[pl.ds(m8((j * 4 + s) * 8), 8), :]
            out[pl.ds(m8(base + 8 * chip + 8 * (1 - core)), 8), :] = other[pl.ds(m8((j * 4 + s) * 8), 8), :]
        for a in range(2):
            both = halo[pl.ds(m8((j * 2 + a) * 8), 8), :]
            turned = pltpu.roll(both, 4, 0)
            out = (edge, inner)[a]
            for si in range(2):
                rows = jnp.where((chip == 0) == (si == 0), both, turned)
                rows = jnp.where(low == (chip == 0), rows, 0.0)
                out[pl.ds(m8((j * 2 + si) * BW + 16 * (1 - chip)), 8), :] = rows
        return carry

    lax.fori_loop(0, 25, step, 0)
    for s in range(4):
        out, base = (edge, inner)[s // 2], (25 * 2 + s % 2) * BW
        out[pl.ds(base, BW), :] = d[pl.ds(m8(plane_of(s, core) * 32 + 8 * chip), BW), :]

    def copy(j, carry):
        for t in range(BW // 8):
            outer[pl.ds(m8(j * BW + 8 * t), 8), :] = edge[pl.ds(m8(j * 2 * BW + 8 * t), 8), :]
        return carry

    lax.fori_loop(0, 26, copy, 0)


def wave_numbers():
    sub = lax.broadcasted_iota(jnp.int32, (8, 128), 0)
    rate = jnp.where(sub < 3, sub + 1, jnp.where(sub < 4, 0, jnp.where(sub < 7, 3 - sub, 0)))
    return rate.astype(F32)


def blocks(place, row, source):
    ref, s, count = place

    def entry(j):
        return ref[pl.ds((j * count + s) * BW + row, 8, stride=0), :]

    outs = []
    for v in range(NV):
        total = entry(v * NV) * source[0]
        for u in range(1, NV):
            total = total + entry(v * NV + u) * source[u]
        outs.append(total)
    return outs


def eight(beyond, edge, inner, across):
    kept = ((beyond, 1), (beyond, 0), (edge, 0), (edge, 1), (inner, 0), (inner, 1), (across, 1), (across, 0))
    return {x: at for x, at in enumerate(kept) if at[0] is not None}


def inverses(beyond, edge, inner, across):
    held = {x: (ref, s, 2) for x, (ref, s) in eight(None, edge, inner, across).items()}
    return held | {1: (beyond, 0, 1)}


def residuals(beyond, edge, inner, across):
    held = eight(None, edge, inner, across)
    return held if beyond is None else held | {1: (beyond, 0)}


def first_solve(planes, chip, resid, inv, write):
    def step(row, carry):
        for x in planes:
            ref, s = resid[x]
            source = [ref[(s * RW + row) * NV + v] for v in range(NV)]
            write(x, row, blocks(inv[x], row + 4 * chip, source))
        return carry

    lax.fori_loop(0, RW, step, 0, unroll=4 if len(planes) > 2 else 10)


def sweep(planes, first, count, chip, resid, inv, update, write):
    lane = lax.broadcasted_iota(jnp.int32, (8, 128), 1)
    inside_low, inside_high = lane > 0, lane < 127
    rate = wave_numbers()

    def at(x, row, v):
        ref, s = update[x]
        return ref[(s * (RW + 2) + row + 1) * NV + v]

    def step(n, carry):
        row = first + n
        before = [at(planes[0] - 1, row, v) for v in range(NV)]
        own = [at(planes[0], row, v) for v in range(NV)]
        for x in planes:
            r_ref, s = resid[x]
            b_ref, b_s, b_count = inv[x]
            weight = b_ref[pl.ds((25 * b_count + b_s) * BW + row + 4 * chip, 8, stride=0), :]
            after = [at(x + 1, row, v) for v in range(NV)]
            source = []
            for v in range(NV):
                w = own[v]
                beside = (before[v] + after[v]) + (at(x, row - 1, v) + at(x, row + 1, v))
                beside = beside + jnp.where(inside_low, pltpu.roll(w, 1, 1), 0.0)
                beside = beside + jnp.where(inside_high, pltpu.roll(w, 127, 1), 0.0)
                turned = r_ref[(s * RW + row) * NV + v] - rate * pltpu.roll(w, 4, 0)
                source.append(turned + weight * beside)
            write(x, row, blocks(inv[x], row + 4 * chip, source))
            before, own = own, after
        return carry

    lax.fori_loop(0, count, step, 0, unroll=count if len(planes) < 3 else count // 2)


def clear_rows(*refs):
    zero = jnp.zeros((8, 128), F32)
    for ref in refs:
        for x in range(ref.shape[0] // ((RW + 2) * NV)):
            for v in range(NV):
                ref[x * (RW + 2) * NV + v] = zero
                ref[(x * (RW + 2) + RW + 1) * NV + v] = zero


def into(update):
    def write(x, row, values):
        ref, s = update[x]
        for v in range(NV):
            ref[(s * (RW + 2) + row + 1) * NV + v] = values[v]

    return write


def into_edge(out, start, chip):
    def write(x, row, values):
        for v in range(NV):
            out[((x - start) * (RW - 2) + row - 2 * chip) * NV + v] = values[v]

    return write


def fill(update, given, chip):
    def step(n, carry):
        for x, (ref, s) in given.items():
            into(update)(x, n + 2 * chip, [ref[(s * (RW - 2) + n) * NV + v] for v in range(NV)])
        return carry

    lax.fori_loop(0, RW - 2, step, 0, unroll=3)


def own_kernel(re, ri, be, bi, k0, k1):
    _, chip = place()
    resid, inv = residuals(None, re, ri, None), inverses(None, be, bi, None)
    zeroth = {x: (k0, x - 2) for x in range(2, 6)}
    clear_rows(k0, k1)
    first_solve(range(2, 6), chip, resid, inv, into(zeroth))
    sweep(range(3, 5), 0, RW, chip, resid, inv, zeroth, into({3: (k1, 0), 4: (k1, 1)}))


def first_inner_kernel(ri, rd, bi, bd, k0, k1, ui, u0, u1):
    _, chip = place()
    resid, inv = residuals(None, None, ri, rd), inverses(None, None, bi, bd)
    zeroth = {4: (k0, 2), 5: (k0, 3), 6: (u0, 0), 7: (u0, 1)}
    oneth = {3: (k1, 0), 4: (k1, 1), 5: (u1, 0), 6: (u1, 1)}
    clear_rows(u0, u1)
    first_solve(range(6, 8), chip, resid, inv, into(zeroth))
    sweep(range(5, 7), 0, RW, chip, resid, inv, zeroth, into(oneth))
    sweep(range(4, 6), 2 * chip, RW - 2, chip, resid, inv, oneth, into_edge(ui, 4, chip))


def first_edge_kernel(cells, rx, re, bx, by, be, k0, k1, ue, sent, rz, bz, u0, u1):
    core, chip = place()
    resid, inv = residuals(rz, re, None, None), inverses(bz, be, None, None)
    zeroth = {0: (u0, 0), 1: (u0, 1), 2: (k0, 0), 3: (k0, 1)}
    oneth = {1: (u1, 0), 2: (u1, 1), 3: (k1, 0), 4: (k1, 1)}
    clear_rows(u0, u1)
    passed_on = lax.axis_index("cells") == jnp.where(core == 0, 0, cells - 1)

    def copy_blocks(j, carry):
        at = pl.ds(m8(j * 8), 8)
        bz[at, :] = by[at, :] + jnp.where(passed_on, 0.0, bx[at, :])
        return carry

    for n in range(RW - 1):
        for v in range(NV):
            rz[(n + chip) * NV + v] = rx[n * NV + v]
    for n in range(RW - 2):
        into(zeroth)(0, n + 2 * chip, [rx[(RW - 1 + n) * NV + v] for v in range(NV)])
    lax.fori_loop(0, 26 * BW // 8, copy_blocks, 0, unroll=6)
    first_solve(range(1, 2), chip, resid, inv, into(zeroth))
    sweep(range(1, 3), 0, RW, chip, resid, inv, zeroth, into(oneth))
    sweep(range(2, 4), 2 * chip, RW - 2, chip, resid, inv, oneth, into_edge(ue, 2, chip))
    for s in range(2):
        for n in range(RW - 3 - s):
            for v in range(NV):
                sent[(s * (RW - 3) + n) * NV + v] = ue[(s * (RW - 2) + n + (1 + s) * chip) * NV + v]


def unpack(last, outs, core, chip):
    def step(v, carry):
        for s in range(2):
            for t in range(2):
                start = (s * 16 + 8 * t) * 40 + v * 8
                values = from_modes([last[pl.ds(start + m, 8, stride=40), :] for m in range(8)])
                pairs = [values[2 * q : 2 * q + 2] for q in range(4)]
                turned = [[jnp.where(core == 1, pairs[q ^ 1][e], pairs[q][e]) for e in range(2)] for q in range(4)]
                for k, out in enumerate(outs):
                    for e in range(2):
                        out[pl.ds(m8(((e * NV + v) * 2 + s) * 16 + 8 * t), 8), :] = jnp.where(
                            chip == 1, turned[k ^ 2][e], turned[k][e]
                        )
        return carry

    lax.fori_loop(0, NV, step, 0)


def into_last(last, start, chip):
    def write(x, row, values):
        for v in range(NV):
            last[pl.ds(m8((((x - start) * 16 + row - 4 * chip) * NV + v) * 8), 8), :] = values[v]

    return write


def second_inner_kernel(re, ri, rd, be, bi, bd, ue, ui, ud, o0, o1, o2, o3, k3, u2, u3, last):
    core, chip = place()
    resid, inv = residuals(None, re, ri, rd), inverses(None, be, bi, bd)
    second = {x: (u2, x - 2) for x in range(2, 8)}
    third = {3: (k3, 0), 4: (k3, 1), 5: (u3, 0), 6: (u3, 1)}
    clear_rows(u2, u3, k3)
    fill(second, eight(None, ue, ui, ud), chip)
    sweep(range(3, 7), 2 * chip, RW - 2, chip, resid, inv, second, into(third))
    sweep(range(4, 6), 4 * chip, RW - 4, chip, resid, inv, third, into_last(last, 4, chip))
    unpack(last, (o0, o1, o2, o3), core, chip)


def second_edge_kernel(rz, re, bx, be, ux, ue, k3, o0, o1, o2, o3, u2, u3, last):
    core, chip = place()
    resid, inv = residuals(rz, re, None, None), inverses(bx, be, None, None)
    second = {x: (u2, x) for x in range(4)}
    third = {1: (u3, 0), 2: (u3, 1), 3: (k3, 0), 4: (k3, 1)}
    clear_rows(u2, u3)
    fill(second, eight(None, ue, None, None), chip)
    for s in range(2):
        for n in range(RW - 3 - s):
            values = [ux[(s * (RW - 3) + n) * NV + v] for v in range(NV)]
            into(second)(1 - s, n + (3 + s) * chip, values)
    sweep(range(1, 3), 2 * chip, RW - 2, chip, resid, inv, second, into(third))
    sweep(range(2, 4), 4 * chip, RW - 4, chip, resid, inv, third, into_last(last, 2, chip))
    unpack(last, (o0, o1, o2, o3), core, chip)


def final_kernel(f, w0, w1, w2, w3, v0, v1, v2, v3, new, out, sent):
    core, chip = place()

    def store(ev):
        at = pl.ds(m8(ev * 256), 256)
        return pltpu.make_async_copy(out.at[at, :], new.at[at, :], sent.at[ev])

    def step(ev, carry):
        for k in range(4):
            for s in range(4):
                w = ((w0, w1, w2, w3), (v0, v1, v2, v3))[s // 2][k]
                base = (ev * 8 + plane_of(s, core ^ (k & 1))) * 32 + 16 * (chip ^ (k >> 1))
                for t in range(2):
                    at = pl.ds(m8(base + 8 * t), 8)
                    out[at, :] = f[at, :] - w[pl.ds(m8((ev * 2 + s % 2) * 16 + 8 * t), 8), :]
        store(ev).start()
        return carry

    lax.fori_loop(0, 10, step, 0)
    for ev in range(10):
        store(ev).wait()


def call(kernel, shapes, *args, scratch=(), **specs):
    return pl.pallas_call(
        kernel,
        out_shape=tuple(jax.ShapeDtypeStruct(s, F32) for s in shapes),
        scratch_shapes=[pltpu.VMEM(s, F32) if isinstance(s, tuple) else s for s in scratch],
        **specs,
        compiler_params=pltpu.CompilerParams(vmem_limit_bytes=40 * 1024 * 1024),
    )(*args)


def exchanges(cells):
    def pairs(move):
        found = []
        for i in range(4):
            for c in range(cells):
                target = move(i, c)
                if target is not None and 0 <= target[1] < cells:
                    found.append((i * cells + c, target[0] * cells + target[1]))
        return found

    def beside(i, c):
        return i ^ 1, c - 1 if i % 2 == 0 else c + 1

    half = cells // 2
    middle, ends = ((0, half), (1, half - 1)), (0, cells - 1)
    return {
        "core": pairs(lambda i, c: (i ^ 1, c)),
        "chip": pairs(lambda i, c: (i ^ 2, c)),
        "both": pairs(lambda i, c: (i ^ 3, c)),
        "up": pairs(lambda i, c: (i, c + 1)),
        "down": pairs(lambda i, c: (i, c - 1)),
        "next": pairs(beside),
        "leg": pairs(lambda i, c: (i ^ 1, ends[i % 2 ^ 1]) if (i % 2, c) in middle else beside(i, c)),
        "relay": pairs(lambda i, c: (i, half - i % 2) if c == ends[i % 2] else None),
    }


def on_device(flow_state, forcing, diffusion, block_inverse):
    routes = exchanges(lax.axis_size("cells"))

    def send(value, route):
        return lax.ppermute(value, AXES, routes[route])

    f = flow_state.reshape(2560, 128)
    g = forcing.reshape(2560, 128)
    d = diffusion.reshape(256, 128)
    b = block_inverse.reshape(1600, 128)

    states = [(800, 128)] * 4 + [(320, 128)] * 2
    f0, f1, f2, f3, low, high = call(state_kernel, states, f)
    f2, f3 = send(f2, "chip"), send(f3, "both")
    lo, hi = send(high, "up"), send(low, "down")
    own, other = call(inverse_pack_kernel, [(800, 128)] * 2, b)
    other = send(other, "core")
    f1 = send(f1, "core")
    (halo,) = call(halo_kernel, [(400, 128)], own, other)
    halo = send(halo, "chip")

    parts = call(part_kernel, [(400, 128)] * 8, f, g, d, lo, hi, scratch=[(2560, 128)])
    e0, e1, e2, e3, i0, i1, i2, i3 = parts
    e2, e3, e1 = send(e2, "chip"), send(e3, "both"), send(e1, "core")
    i2, i3, i1 = send(i2, "chip"), send(i3, "both"), send(i1, "core")

    windows = [(26 * 2 * BW, 128)] * 2 + [(26 * BW, 128)]
    be, bi, bx = call(inverse_window_kernel, windows, own, other, halo, d)
    bx, bd = send(bx, "leg"), send(bi, "core")

    r_shape = (2 * RW * 40, 128)
    re, rx = call(edge_kernel, [r_shape, ((2 * RW - 3) * 40, 128)], f0, f1, f2, f3, e0, e1, e2, e3, be)
    rx = send(rx, "next")
    by = send(bx, "relay")
    (ri,) = call(lambda *refs: modes_kernel(400, *refs), [r_shape], f0, f1, f2, f3, i0, i1, i2, i3)
    rd = send(ri, "core")
    rx, re, ri, rd = (r.reshape(-1, 8, 128) for r in (rx, re, ri, rd))

    def planes(count):
        return (count * (RW + 2) * NV, 8, 128)

    u_shape, last = (2 * (RW - 2) * NV, 8, 128), (2 * 16 * 40, 128)
    k0, k1 = call(own_kernel, [planes(4), planes(2)], re, ri, be, bi)
    (ui,) = call(first_inner_kernel, [u_shape], ri, rd, bi, bd, k0, k1, scratch=[planes(2), planes(2)])
    ud = send(ui, "core")
    cells = lax.axis_size("cells")
    ue, ux, rz, bx = call(
        lambda *refs: first_edge_kernel(cells, *refs),
        [u_shape, ((2 * RW - 7) * NV, 8, 128), (RW * NV, 8, 128), (26 * BW, 128)],
        *(rx, re, bx, by, be, k0, k1),
        scratch=[planes(2), planes(2)],
    )
    ux = send(ux, "next")
    v0, v1, v2, v3, k3 = call(
        second_inner_kernel,
        [(320, 128)] * 4 + [planes(2)],
        *(re, ri, rd, be, bi, bd, ue, ui, ud),
        scratch=[planes(6), planes(2), last],
    )
    v2, v3, v1 = send(v2, "chip"), send(v3, "both"), send(v1, "core")
    w0, w1, w2, w3 = call(
        second_edge_kernel, [(320, 128)] * 4, *(rz, re, bx, be, ux, ue, k3), scratch=[planes(4), planes(2), last]
    )
    w2, w3, w1 = send(w2, "chip"), send(w3, "both"), send(w1, "core")
    copies = [(2560, 128), pltpu.SemaphoreType.DMA((10,))]
    hbm = pl.BlockSpec(memory_space=pltpu.HBM)
    (out,) = call(final_kernel, [(2560, 128)], f, w0, w1, w2, w3, v0, v1, v2, v3, scratch=copies, out_specs=(hbm,))
    return out.reshape(flow_state.shape)


def solution(mesh):
    in_specs = (
        P("inst", None, "cells", None, None),
        P("inst", None, "cells", None, None),
        P("cells", None, None),
        P(None, None, "cells", "inst", None),
    )
    out_specs = P("inst", None, "cells", None, None)
    return jax.shard_map(
        on_device, mesh=mesh, in_specs=in_specs, out_specs=out_specs, check_vma=False
    )
```
